32 devices in a mesh: ga: 8 (over y, x, core), band: 4 (over z).
Axes of the slice: x: 2, y: 2, z: 4, core: 2. Of those that a mesh axis runs over, the one named last changes fastest.
Arguments:
- psi: bfloat16 [2, 8, 96, 2048], P(None, 'band', None, 'ga'), may hold values from -6 to 6
- vloc: float32 [96, 9216], P('ga'), may hold values from 0.5 to 1.5
- dv: float32 [96, 9216], P('ga'), may hold values from -6 to 6
- beta: float32 [2, 128, 96, 2048], P(None, None, None, 'ga'), may hold values from -0.02734375 to 0.02734375
- dij: float32 [2, 4, 4], replicated, may hold values from -1 to 1.5, as said below
- atom_type: int32 [32], replicated, may hold values from 0 to 1
- stick_xy: int32 [2048], replicated, may hold values from 0 to 9215, as said below
- band_shift: float32 [8], P('band'), may hold values from 0.3 to 3
Outputs:
- response: float32 [2, 8, 96, 2048], P(None, 'band', None, 'ga')
- density: float32 [96, 9216], P('ga', 'band')
The draws below stay inside these ranges and needn't reach their ends.
Inputs may be any that keep to these rules, and one draw needn't show every extreme that they name: `stick_xy`: 2048 distinct columns, each with both frequencies f(y) and f(x) in -(32) to 31. `dij`: each of the 2 matrices is symmetric positive definite with diagonal at least 0.5.
All inputs are finite; a program needn't handle non-finite values.
Results may differ from the reference program's by a relative error of at most 0.0003.
Values may be sent and summed in bfloat16 or wider, within the bound.
No kernel may reach another device: no remote copies, remote signals or barrier semaphores. Data moves between devices by JAX's collectives and lax.ppermute only.
A program may use at most 128 MiB of HBM per device.

```python
import math
import jax
import jax.numpy as jnp
from jax import lax

GRID = 96
STICKS = 2048
NATOM = 32
NBETA = 4
NTYPE = 2
ITERS = 2
NPROJ = 128
BANDS = 8


def draw_stick_xy(key, part):
    radius_cells = GRID // 3
    square_side = 2 * radius_cells
    chosen = jax.random.permutation(key, square_side * square_side)[:STICKS]
    freq_y = chosen // square_side - radius_cells
    freq_x = chosen % square_side - radius_cells
    return (freq_y % GRID * GRID + freq_x % GRID).astype(jnp.int32)


def draw_dij(key, part):
    factor = jax.random.uniform(key, (NTYPE, NBETA, NBETA), jnp.float32, -1.0, 1.0)
    product = jnp.einsum('tij,tkj->tik', factor, factor) / NBETA
    return product + 0.5 * jnp.eye(NBETA, dtype=jnp.float32)[None]


def with_ends(values, key, least, largest):
    dims = values.shape
    spot = [jax.random.randint(jax.random.fold_in(key, axis), (), 0, dims[axis]) for axis in range(len(dims))]
    values = values.at[tuple(spot)].set(least)
    longest = dims.index(max(dims))
    spot[longest] = (spot[longest] + 1) % dims[longest]
    return values.at[tuple(spot)].set(largest)


def level_of(key, dims, cuts, low, high):
    gain = 1.0
    for dim, parts in cuts:
        draws = jax.random.uniform(jax.random.fold_in(jax.random.fold_in(key, 6), dim), (parts,), jnp.float32, low / len(cuts), high / len(cuts))
        gain = gain * jnp.repeat(jnp.exp(draws), dims[dim] // parts).reshape((-1,) + (1,) * (len(dims) - 1 - dim))
    return gain


def noise(rng, dims, width, reach, shards=(), kind=jnp.bfloat16):
    entries = jax.random.normal(rng, dims, jnp.float32) * width
    if len(shards) > 0:
        entries = level_of(rng, dims, shards, -0.22, 0.18) * entries
    return jnp.clip(entries, min=-reach, max=reach).astype(kind)


def setup_inputs(seed: int = 0) -> dict:
    streams_of = jax.random.split(jax.random.key(seed), 9)
    return {
        "psi": noise(streams_of[0], (2, BANDS, GRID, STICKS), 1.0, 6.0, ((1, 4), (3, 8))),
        "vloc": jnp.clip(0.5 + 1.0 * jax.random.uniform(streams_of[1], (GRID, GRID * GRID), jnp.float32) ** level_of(streams_of[1], (GRID, GRID * GRID), ((0, 8),), -0.2, 0.2), 0.5, 1.5),
        "dv": noise(streams_of[2], (GRID, GRID * GRID), 1.0, 6.0, ((0, 8),), jnp.float32),
        "beta": noise(streams_of[3], (2, NPROJ, GRID, STICKS), (GRID * STICKS // 4) ** -0.5, 0.02734375, ((3, 8),), jnp.float32),
        "dij": draw_dij(jax.random.fold_in(streams_of[8], 71), 0),
        "atom_type": with_ends(jax.random.randint(streams_of[5], (NATOM,), 0, NTYPE), jax.random.fold_in(streams_of[5], 1), 0, NTYPE - 1).astype(jnp.int32),
        "stick_xy": draw_stick_xy(jax.random.fold_in(streams_of[8], 71), 0),
        "band_shift": jnp.clip(jnp.exp(math.log(3.0) - 2.3025851 * jax.random.uniform(streams_of[7], (BANDS,), jnp.float32) ** level_of(streams_of[7], (BANDS,), ((0, 4),), -0.2, 0.2)), 0.3, 3.0),
    }


highest = lax.Precision.HIGHEST


def frequency(index):
    return (index + GRID // 2) % GRID - GRID // 2


def kinetic_table(stick_xy):
    freq_z = frequency(jnp.arange(GRID, dtype=jnp.int32))
    freq_y = frequency(stick_xy // GRID)
    freq_x = frequency(stick_xy % GRID)
    summed = freq_z[:, None] ** 2 + (freq_y ** 2 + freq_x ** 2)[None, :]
    return summed.astype(jnp.float32) * (4.0 / (GRID * GRID))


def to_real(coef, stick_xy):
    values = coef[0] + 1j * coef[1]
    grid = jnp.zeros((GRID, GRID * GRID), values.dtype).at[:, stick_xy].set(values)
    field = jnp.fft.ifftn(grid.reshape(GRID, GRID, GRID)) * (GRID ** 1.5)
    field = field.reshape(GRID, GRID * GRID)
    return jnp.stack([jnp.real(field), jnp.imag(field)])


def to_recip(field, stick_xy):
    values = (field[0] + 1j * field[1]).reshape(GRID, GRID, GRID)
    spectrum = jnp.fft.fftn(values).reshape(GRID, GRID * GRID) / (GRID ** 1.5)
    picked = spectrum[:, stick_xy]
    return jnp.stack([jnp.real(picked), jnp.imag(picked)])


def reference(psi, vloc, dv, beta, dij, atom_type, stick_xy, band_shift):
    occupied = jnp.moveaxis(psi.astype(jnp.float32), 1, 0)
    kinetic = kinetic_table(stick_xy)
    inv_norm = 1.0 / (2.0 * GRID * STICKS)

    def dv_image(coef):
        return to_recip(dv[None] * to_real(coef, stick_xy), stick_xy)

    image = lax.map(dv_image, occupied)
    intersect_re = jnp.einsum('mczs,nczs->mn', occupied, image, precision=highest) * inv_norm
    intersect_im = (jnp.einsum('mzs,nzs->mn', occupied[:, 0], image[:, 1], precision=highest) - jnp.einsum('mzs,nzs->mn', occupied[:, 1], image[:, 0], precision=highest)) * inv_norm
    corr_re = jnp.einsum('mn,mzs->nzs', intersect_re, occupied[:, 0], precision=highest) - jnp.einsum('mn,mzs->nzs', intersect_im, occupied[:, 1], precision=highest)
    corr_im = jnp.einsum('mn,mzs->nzs', intersect_im, occupied[:, 0], precision=highest) + jnp.einsum('mn,mzs->nzs', intersect_re, occupied[:, 1], precision=highest)
    rhs = jnp.stack([corr_re, corr_im], axis=1) - image
    selected = dij[atom_type]
    diagonal = kinetic[None] + band_shift[:, None, None]

    def local_image(coef):
        return to_recip(vloc[None] * to_real(coef, stick_xy), stick_xy)

    def apply_operator(vector):
        local = lax.map(local_image, vector)
        proj_re = jnp.einsum('jzs,bzs->bj', beta[0], vector[:, 0], precision=highest) + jnp.einsum('jzs,bzs->bj', beta[1], vector[:, 1], precision=highest)
        proj_im = jnp.einsum('jzs,bzs->bj', beta[0], vector[:, 1], precision=highest) - jnp.einsum('jzs,bzs->bj', beta[1], vector[:, 0], precision=highest)
        shaped_re = proj_re.reshape(BANDS, NATOM, NBETA)
        shaped_im = proj_im.reshape(BANDS, NATOM, NBETA)
        coup_re = jnp.einsum('aij,baj->bai', selected, shaped_re, precision=highest).reshape(BANDS, NPROJ)
        coup_im = jnp.einsum('aij,baj->bai', selected, shaped_im, precision=highest).reshape(BANDS, NPROJ)
        back_re = jnp.einsum('jzs,bj->bzs', beta[0], coup_re, precision=highest) - jnp.einsum('jzs,bj->bzs', beta[1], coup_im, precision=highest)
        back_im = jnp.einsum('jzs,bj->bzs', beta[0], coup_im, precision=highest) + jnp.einsum('jzs,bj->bzs', beta[1], coup_re, precision=highest)
        return diagonal[:, None] * vector + local + jnp.stack([back_re, back_im], axis=1)

    def band_sum(first, second):
        return jnp.sum(first * second, axis=(1, 2, 3))

    solution = jnp.zeros_like(rhs)
    residual = rhs
    direction = rhs
    norm_now = band_sum(rhs, rhs)
    for iteration in range(ITERS):
        image_now = apply_operator(direction)
        alpha = (norm_now / band_sum(direction, image_now))[:, None, None, None]
        solution = solution + alpha * direction
        residual = residual - alpha * image_now
        if iteration + 1 < ITERS:
            norm_next = band_sum(residual, residual)
            direction = residual + (norm_next / norm_now)[:, None, None, None] * direction
            norm_now = norm_next

    def accumulate(carry, pair):
        psi_field = to_real(pair[0], stick_xy)
        resp_field = to_real(pair[1], stick_xy)
        return carry + 4.0 * jnp.sum(psi_field * resp_field, axis=0), None

    density, unused = lax.scan(accumulate, jnp.zeros((GRID, GRID * GRID), jnp.float32), (occupied, solution))
    return jnp.moveaxis(solution, 0, 1), density
```

```python
import functools

import jax
import jax.numpy as jnp
import numpy as np
from jax import lax
from jax.experimental import pallas as pl
from jax.experimental.pallas import tpu as pltpu
from jax.sharding import PartitionSpec as P

GRID = 96
ITERS = 2
SIDE = 2 * (GRID // 3)
LANES = 128
f32 = jnp.float32
bf16 = jnp.bfloat16
highest = lax.Precision.HIGHEST


def split_const(table):
    table = np.asarray(table, np.float32)
    high = table.astype(jnp.bfloat16)
    low = (table - high.astype(np.float32)).astype(jnp.bfloat16)
    return high, low


def phases(rows, cols):
    angle = (np.outer(rows, cols) % GRID) * (2.0 * np.pi / GRID)
    return np.cos(angle) / np.sqrt(GRID), np.sin(angle) / np.sqrt(GRID)


def z_table(bands):
    cos, sin = phases(np.arange(GRID), np.arange(GRID))
    table = np.zeros((GRID, bands, 2, 2, bands, GRID))
    for b in range(bands):
        table[:, b, 0, 0, b] = cos
        table[:, b, 0, 1, b] = -sin
        table[:, b, 1, 0, b] = sin
        table[:, b, 1, 1, b] = cos
    return table.reshape(GRID * bands * 2, 2 * bands * GRID)


def square_freqs():
    return (np.arange(SIDE) - SIDE // 2) % GRID


def y_table():
    cos, sin = phases(np.arange(GRID), square_freqs())
    return np.block([[cos, -sin], [sin, cos]])


def x_table():
    cos, sin = phases(square_freqs(), np.arange(GRID))
    table = np.zeros((SIDE, 2 * LANES))
    table[:, :GRID] = cos
    table[:, LANES : LANES + GRID] = sin
    return table


def x_back_table():
    cos, sin = phases(np.arange(GRID), square_freqs())
    table = np.zeros((LANES, 4 * SIDE))
    table[:GRID] = np.concatenate([cos, cos, sin, sin], axis=1)
    return table


def split(x):
    high = x.astype(bf16)
    return high, (x - high.astype(f32)).astype(bf16)


def dot(a, b):
    return jnp.dot(a, b, preferred_element_type=f32)


def left(table_hi, table_lo, x):
    high, low = split(x)
    return dot(table_hi, high) + (dot(table_hi, low) + dot(table_lo, high))


def right(x, table_hi, table_lo):
    high, low = split(x)
    return dot(high, table_hi) + (dot(low, table_hi) + dot(high, table_lo))


def params(grid_dims=0):
    semantics = ("arbitrary",) * grid_dims if grid_dims else None
    return pltpu.CompilerParams(
        vmem_limit_bytes=56 * 1024 * 1024, dimension_semantics=semantics
    )


def z_inverse_kernel(coef, t_hi, t_lo, out):
    value = coef[...]
    out[...] = dot(t_hi[...], value) + dot(t_lo[...], value)


def z_inverse(coef, table):
    return pl.pallas_call(
        z_inverse_kernel,
        out_shape=jax.ShapeDtypeStruct(coef.shape, f32),
        compiler_params=params(),
        name="z_inverse",
    )(coef, *table)


def intersect_kernel(bands, recv, occ, b_hi, b_lo, image, parts):
    image[...] = left(b_hi[...], b_lo[...], recv[...])
    total = occ.shape[0] * bands
    sticks = recv.shape[1]

    def lanes(x):
        row = jnp.sum(x, axis=0, keepdims=True)
        return sum(row[:, k : k + LANES] for k in range(0, sticks, LANES))

    for n in range(bands):
        re = image[n * GRID : (n + 1) * GRID, :]
        im = image[(bands + n) * GRID : (bands + n + 1) * GRID, :]
        for m in range(total):
            group, own = m // bands, m % bands
            o_re = occ[group, 0, own].astype(f32)
            o_im = occ[group, 1, own].astype(f32)
            at = m * bands + n
            parts[at : at + 1, :] = lanes(o_re * re + o_im * im)
            at = at + total * bands
            parts[at : at + 1, :] = lanes(o_re * im - o_im * re)


def planes_kernel(mode, bands, recv, pot, row, col1, col2, xt_hi, xt_lo, yt_hi, yt_lo, yb_hi, yb_lo, xb_hi, xb_lo, *rest):
    groups, rows, sticks = recv.shape
    planes = rows // (2 * bands)
    count = planes * bands
    rest = list(rest)
    if mode == "next":
        first, psi_field, ratio = rest[:3]
        rest = rest[3:]
    if mode == "local":
        psi_field = rest[0]
        rest = rest[1:]
    spread = rest[-1]
    for g in range(groups):
        at = g * sticks
        mask = row[:, at : at + sticks]
        value = recv[g]
        high = value.astype(bf16).astype(f32)
        low = value - high
        for part, piece in enumerate((high, low)):
            for r in range(rows):
                to = (part * rows + r) * SIDE
                spread[to : to + SIDE, at : at + sticks] = (mask * piece[r : r + 1, :]).astype(bf16)
    both = dot(spread[...], col1[...])
    half = rows * SIDE
    square = both[:half] + both[half:]
    wide = right(square, xt_hi[...], xt_lo[...])
    fields = []
    for n in range(count):
        re = wide[(2 * n) * SIDE : (2 * n + 1) * SIDE]
        im = wide[(2 * n + 1) * SIDE : (2 * n + 2) * SIDE]
        fields.append(
            jnp.concatenate([re[:, :LANES] - im[:, LANES:], re[:, LANES:] + im[:, :LANES]], axis=0)
        )
    field = left(yt_hi[...], yt_lo[...], jnp.concatenate(fields, axis=1))
    if mode == "next":
        quad, dens = rest[:2]
    elif mode == "local":
        field_out, quad, dens, back = rest[:4]
        field_out[0] = field
    else:
        field_out, back = rest[:2]
        field_out[0] = field
    if mode != "dv":
        sums = [jnp.zeros((1, LANES), f32) for _ in range(bands)]
    products = []
    for n in range(count):
        p, b = n // bands, n % bands
        at = n * LANES
        re = field[:GRID, at : at + LANES]
        im = field[GRID:, at : at + LANES]
        v = pot[p]
        if mode == "next":
            re = re + ratio[b] * first[0, :GRID, at : at + LANES]
            im = im + ratio[b] * first[0, GRID:, at : at + LANES]
        v_re, v_im = v * re, v * im
        if mode != "dv":
            dens[p, b] = (
                psi_field[0, :GRID, at : at + LANES] * re + psi_field[0, GRID:, at : at + LANES] * im
            )
            sums[b] = sums[b] + jnp.sum(v_re * re + v_im * im, axis=0, keepdims=True)
        products.append(jnp.concatenate([v_re, v_im], axis=0))
    if mode != "dv":
        quad[0] = jnp.concatenate(sums, axis=0)
    if mode == "next":
        return
    columns = left(yb_hi[...], yb_lo[...], jnp.concatenate(products, axis=1))
    stacked = jnp.concatenate([columns[:, n * LANES : (n + 1) * LANES] for n in range(count)], axis=0)
    wide = right(stacked, xb_hi[...], xb_lo[...])
    squares = []
    for n in range(count):
        re = wide[(2 * n) * SIDE : (2 * n + 1) * SIDE]
        im = wide[(2 * n + 1) * SIDE : (2 * n + 2) * SIDE]
        squares += [re[:, :LANES] + im[:, LANES:], im[:, :LANES] - re[:, LANES:]]
    square = jnp.concatenate(squares, axis=0)
    high = square.astype(bf16).astype(f32)
    lane = lax.broadcasted_iota(jnp.int32, square.shape, 1)
    pair = jnp.where(lane < SIDE, high, square - high).astype(bf16)
    for g in range(groups):
        at = g * sticks
        mask = row[:, at : at + sticks]
        by_row = dot(pair, col2[:, at : at + sticks])
        for r in range(rows):
            back[g, r : r + 1, :] = jnp.sum(
                by_row[r * SIDE : (r + 1) * SIDE] * mask, axis=0, keepdims=True
            )


def planes_call(mode, recv, pot, maps, tables, groups, bands, extra=()):
    rows, sticks = recv.shape
    recv = recv.reshape(groups, rows // groups, sticks)
    local = recv.shape[1]
    planes = local // (2 * bands)
    step = max(1, 8 // (2 * bands))
    if planes % step:
        step = planes
    steps = planes // step
    width = step * bands * LANES
    whole = lambda a: pl.BlockSpec(a.shape, lambda i: (0,) * a.ndim)
    sticks_spec = pl.BlockSpec((groups, step * 2 * bands, sticks), lambda i: (0, i, 0))
    field_spec = pl.BlockSpec((1, 2 * GRID, width), lambda i: (i, 0, 0))
    field_shape = jax.ShapeDtypeStruct((steps, 2 * GRID, width), f32)
    quad_spec = pl.BlockSpec((1, bands, LANES), lambda i: (i, 0, 0))
    quad_shape = jax.ShapeDtypeStruct((steps, bands, LANES), f32)
    dens_spec = pl.BlockSpec((step, bands, GRID, LANES), lambda i: (i, 0, 0, 0))
    dens_shape = jax.ShapeDtypeStruct((planes, bands, GRID, LANES), f32)
    back_shape = jax.ShapeDtypeStruct(recv.shape, f32)
    in_specs = [sticks_spec, pl.BlockSpec((step, GRID, LANES), lambda i: (i, 0, 0))]
    in_specs += [whole(a) for a in maps] + [whole(a) for a in tables]
    if mode == "dv":
        out_specs, out_shape = [field_spec, sticks_spec], [field_shape, back_shape]
    elif mode == "local":
        in_specs += [field_spec]
        out_specs = [field_spec, quad_spec, dens_spec, sticks_spec]
        out_shape = [field_shape, quad_shape, dens_shape, back_shape]
    else:
        in_specs += [field_spec, field_spec, pl.BlockSpec(memory_space=pltpu.SMEM)]
        out_specs, out_shape = [quad_spec, dens_spec], [quad_shape, dens_shape]
    result = pl.pallas_call(
        functools.partial(planes_kernel, mode, bands),
        grid=(steps,),
        in_specs=in_specs,
        out_specs=out_specs,
        out_shape=out_shape,
        scratch_shapes=[pltpu.VMEM((2 * step * 2 * bands * SIDE, groups * sticks), bf16)],
        compiler_params=params(1),
        name="planes_" + mode,
    )(recv, pot, *maps, *tables, *extra)
    if mode != "next":
        result = list(result)
        result[-1] = result[-1].reshape(rows, sticks)
    return result


def project(beta, vector, bands, acc, chunk):
    count = beta.shape[1]

    def fold(x):
        parts = [x[k : k + 8, l : l + LANES] for k in range(0, x.shape[0], 8) for l in range(0, x.shape[1], LANES)]
        while len(parts) > 1:
            parts = [sum(parts[k : k + 2][1:], parts[k]) for k in range(0, len(parts), 2)]
        return parts[0]

    def body(k, carry):
        for u in range(chunk):
            j = k * chunk + u
            b_re, b_im = beta[0, j], beta[1, j]
            for b in range(bands):
                re, im = vector[0][b], vector[1][b]
                acc[j, b] += fold(b_re * re + b_im * im)
                acc[j, bands + b] += fold(b_re * im - b_im * re)
        return carry

    lax.fori_loop(0, count // chunk, body, 0)


def emit(acc, projected, vec, out, t_hi, t_lo):
    projected[...] = jnp.sum(acc[...], axis=2)
    out[...] = left(t_hi[...], t_lo[...], vec[...])


def tile_sums(x):
    row = jnp.sum(x, axis=0, keepdims=True)
    return sum(row[:, k : k + LANES] for k in range(0, x.shape[1], LANES))


def rhs_kernel(bands, parts, occ, image, diag, beta, t_hi, t_lo, vec_out, stats, projected, out, vec, acc):
    step = pl.program_id(0)
    last = pl.num_programs(0) - 1
    zt = image.shape[2]
    total = occ.shape[0] * bands

    @pl.when(step == 0)
    def _():
        acc[...] = jnp.zeros_like(acc)
        stats[...] = jnp.zeros_like(stats)

    vector = [[], []]
    for n in range(bands):
        re, im = -image[0, n], -image[1, n]
        for m in range(total):
            group, own = m // bands, m % bands
            o_re = occ[group, 0, own].astype(f32)
            o_im = occ[group, 1, own].astype(f32)
            at = m * bands + n
            i_re = parts[0, at]
            i_im = parts[0, at + total * bands]
            re = re + (o_re * i_re - o_im * i_im)
            im = im + (o_re * i_im + o_im * i_re)
        vector[0].append(re)
        vector[1].append(im)
    for n in range(bands):
        d = diag[n]
        sq = vector[0][n] * vector[0][n] + vector[1][n] * vector[1][n]
        stats[0, n : n + 1, :] += tile_sums(sq)
        stats[1, n : n + 1, :] += tile_sums(d * sq)
        for c in range(2):
            vec_out[c, n] = vector[c][n]
            vec[pl.ds((c * bands + n) * GRID + step * zt, zt), :] = vector[c][n]
    project(beta, vector, bands, acc, 4)

    @pl.when(step == last)
    def _():
        emit(acc, projected, vec, out, t_hi, t_lo)


def update_kernel(bands, coupled, alpha, recv, p0, diag, beta, b_hi, b_lo, t_hi, t_lo, vec_out, stats, projected, out, vec, local, acc):
    step = pl.program_id(0)
    last = pl.num_programs(0) - 1
    zt = p0.shape[2]

    @pl.when(step == 0)
    def _():
        acc[...] = jnp.zeros_like(acc)
        stats[...] = jnp.zeros_like(stats)
        local[...] = left(b_hi[...], b_lo[...], recv[...])

    first = []
    for c in range(2):
        for n in range(bands):
            at = pl.multiple_of((c * bands + n) * GRID + step * zt, 8)
            first.append(diag[n] * p0[c, n] + local[pl.ds(at, zt), :])

    def body(k, carry):
        for u in range(2):
            j = k * 2 + u
            b_re, b_im = beta[0, j], beta[1, j]
            new = [None] * (2 * bands)
            for n in range(bands):
                w_re, w_im = coupled[n, j], coupled[bands + n, j]
                new[n] = carry[n] + (b_re * w_re - b_im * w_im)
                new[bands + n] = carry[bands + n] + (b_re * w_im + b_im * w_re)
            carry = tuple(new)
        return carry

    image = lax.fori_loop(0, beta.shape[1] // 2, body, tuple(first))
    vector = [[], []]
    for c in range(2):
        for n in range(bands):
            value = p0[c, n] - alpha[n] * image[c * bands + n]
            vector[c].append(value)
            vec_out[c, n] = value
            at = pl.multiple_of((c * bands + n) * GRID + step * zt, 8)
            vec[pl.ds(at, zt), :] = value
    for n in range(bands):
        d = diag[n]
        sq = vector[0][n] * vector[0][n] + vector[1][n] * vector[1][n]
        cross = vector[0][n] * p0[0, n] + vector[1][n] * p0[1, n]
        stats[0, n : n + 1, :] += tile_sums(sq)
        stats[1, n : n + 1, :] += tile_sums(d * sq)
        stats[2, n : n + 1, :] += tile_sums(d * cross)
    project(beta, vector, bands, acc, 4)

    @pl.when(step == last)
    def _():
        emit(acc, projected, vec, out, t_hi, t_lo)


def frequency(index):
    return (index + GRID // 2) % GRID - GRID // 2


def per_device(psi, vloc, dv, beta, dij, atom_type, stick_xy, band_shift, *, groups):
    bands, sticks = psi.shape[1], psi.shape[3]
    nproj = beta.shape[1]
    planes = vloc.shape[0]
    all_sticks = stick_xy.shape[0]
    flat = (2 * bands * GRID, sticks)
    shaped = (2, bands, GRID, sticks)
    table = z_table(bands)
    t_inv = [jnp.asarray(a) for a in split_const(table)]
    t_fwd = [jnp.asarray(a) for a in split_const(table.T)]
    tables = []
    for item in (x_table(), y_table(), y_table().T, x_back_table()):
        tables += [jnp.asarray(a) for a in split_const(item)]
    slots = jnp.arange(SIDE, dtype=jnp.int32)
    row_slot = frequency(stick_xy // GRID) + SIDE // 2
    col_slot = frequency(stick_xy % GRID) + SIDE // 2
    row_hot = (slots[:, None] == row_slot[None, :]).astype(f32)
    col_hot = (col_slot[:, None] == slots[None, :]).astype(bf16)
    twice = jnp.arange(2 * SIDE, dtype=jnp.int32) % SIDE
    col_twice = (twice[:, None] == col_slot[None, :]).astype(bf16)
    maps = (row_hot, col_hot, col_twice)

    def grid_of(field):
        return jnp.pad(field.reshape(planes, GRID, GRID), ((0, 0), (0, 0), (0, LANES - GRID)))

    def swap(x):
        return lax.all_to_all(x, "ga", split_axis=0, concat_axis=0, tiled=True)

    start = lax.axis_index("ga") * sticks
    own_xy = lax.dynamic_slice_in_dim(stick_xy, start, sticks)
    freq_z = frequency(jnp.arange(GRID, dtype=jnp.int32))
    summed = (
        freq_z[:, None] ** 2
        + (frequency(own_xy // GRID) ** 2 + frequency(own_xy % GRID) ** 2)[None, :]
    )
    kinetic = summed.astype(f32) * (4.0 / (GRID * GRID))
    diag = kinetic[None] + band_shift[:, None, None]
    onehot = (atom_type[:, None] == jnp.arange(dij.shape[0], dtype=jnp.int32)[None, :]).astype(f32)
    selected = jnp.einsum("at,tij->aij", onehot, dij, precision=highest)

    def couple(projected):
        parts = projected.reshape(2 * bands, selected.shape[0], selected.shape[1])
        return jnp.einsum("aij,caj->cai", selected, parts, precision=highest).reshape(2 * bands, nproj)

    occ = lax.all_gather(psi, "band", axis=0)
    dv_grid, vloc_grid = grid_of(dv), grid_of(vloc)
    along = swap(z_inverse(psi.reshape(flat), t_inv))
    psi_field, back = planes_call("dv", along, dv_grid, maps, tables, groups, bands)
    pairs = 2 * occ.shape[0] * bands * bands
    image, parts = pl.pallas_call(
        functools.partial(intersect_kernel, bands),
        out_shape=[jax.ShapeDtypeStruct(flat, f32), jax.ShapeDtypeStruct((pairs, LANES), f32)],
        compiler_params=params(),
        name="intersects",
    )(swap(back), occ, *t_fwd)
    inv_norm = 1.0 / (2.0 * GRID * all_sticks)
    intersect = (lax.psum(jnp.sum(parts, axis=1), "ga") * inv_norm)[None]

    zt = 16
    steps = GRID // zt
    whole = lambda a: pl.BlockSpec(a.shape, lambda i: (0,) * a.ndim)
    smem = pl.BlockSpec(memory_space=pltpu.SMEM)
    vec_spec = pl.BlockSpec((2, bands, zt, sticks), lambda i: (0, 0, i, 0))
    occ_spec = pl.BlockSpec((occ.shape[0], 2, bands, zt, sticks), lambda i: (0, 0, 0, i, 0))
    diag_spec = pl.BlockSpec((bands, zt, sticks), lambda i: (0, i, 0))
    beta_spec = pl.BlockSpec((2, nproj, zt, sticks), lambda i: (0, 0, i, 0))
    stats_shape = jax.ShapeDtypeStruct((3, bands, LANES), f32)
    proj_shape = jax.ShapeDtypeStruct((nproj, 2 * bands, LANES), f32)
    flat_shape = jax.ShapeDtypeStruct(flat, f32)
    outs = [jax.ShapeDtypeStruct(shaped, f32), stats_shape, proj_shape, flat_shape]
    out_specs = [vec_spec, whole(stats_shape), whole(proj_shape), whole(flat_shape)]
    acc_scratch = pltpu.VMEM((nproj, 2 * bands, 8, LANES), f32)

    p0, stats0, proj0, along = pl.pallas_call(
        functools.partial(rhs_kernel, bands),
        grid=(steps,),
        in_specs=[smem, occ_spec, vec_spec, diag_spec, beta_spec, whole(t_inv[0]), whole(t_inv[1])],
        out_specs=out_specs,
        out_shape=outs,
        scratch_shapes=[pltpu.VMEM(flat, f32), acc_scratch],
        compiler_params=params(1),
        name="rhs",
    )(intersect, occ, image.reshape(shaped), diag, beta, *t_inv)
    p0_field, quad0, dens0, back = planes_call(
        "local", swap(along), vloc_grid, maps, tables, groups, bands, (psi_field,)
    )
    stats0, proj0, quad0 = lax.psum(
        (jnp.sum(stats0, axis=2), jnp.sum(proj0, axis=2).T, jnp.sum(quad0, axis=(0, 2))), "ga"
    )
    coupled0 = couple(proj0)

    def band_dot(a, b):
        return jnp.sum((a * b).reshape(2, bands, nproj), axis=(0, 2))

    rr0 = stats0[0]
    alpha0 = rr0 / (stats0[1] + quad0 + band_dot(proj0, coupled0))
    r1, stats1, proj1, along = pl.pallas_call(
        functools.partial(update_kernel, bands),
        grid=(steps,),
        in_specs=[smem, smem, whole(flat_shape), vec_spec, diag_spec, beta_spec]
        + [whole(t_inv[0])] * 4,
        out_specs=out_specs,
        out_shape=outs,
        scratch_shapes=[pltpu.VMEM(flat, f32), pltpu.VMEM(flat, f32), acc_scratch],
        compiler_params=params(1),
        name="update",
    )(coupled0, alpha0, swap(back), p0, diag, beta, *t_fwd, *t_inv)
    stats1, proj1 = lax.psum((jnp.sum(stats1, axis=2), jnp.sum(proj1, axis=2).T), "ga")
    ratio = stats1[0] / rr0
    quad1, dens1 = planes_call(
        "next", swap(along), vloc_grid, maps, tables, groups, bands, (p0_field, psi_field, ratio)
    )
    quad1 = lax.psum(jnp.sum(quad1, axis=(0, 2)), "ga")
    spread_ratio = jnp.tile(ratio, 2)[:, None]
    proj_p1 = proj1 + spread_ratio * proj0
    diag1 = stats1[1] + ratio * (2.0 * stats1[2] + ratio * stats0[1])
    alpha1 = stats1[0] / (diag1 + quad1 + band_dot(proj_p1, couple(proj_p1)))
    wide = lambda a: a[None, :, None, None]
    response = wide(alpha1) * r1 + wide(alpha0 + alpha1 * ratio) * p0
    contribution = 4.0 * jnp.sum(wide(alpha0) * dens0 + wide(alpha1) * dens1, axis=1)
    density = lax.psum_scatter(contribution, "band", scatter_dimension=1, tiled=True)
    return response, density[:, :, :GRID].reshape(planes, -1)


def solution(mesh):
    placed = (
        P(None, "band", None, "ga"),
        P("ga", None),
        P("ga", None),
        P(None, None, None, "ga"),
        P(),
        P(),
        P(),
        P("band"),
    )
    return jax.shard_map(
        functools.partial(per_device, groups=mesh.shape["ga"]),
        mesh=mesh,
        in_specs=placed,
        out_specs=(P(None, "band", None, "ga"), P("ga", "band")),
        check_vma=False,
    )
```

```python
import functools

import jax
import jax.numpy as jnp
import numpy as np
from jax import lax
from jax.experimental import pallas as pl
from jax.experimental.pallas import tpu as pltpu
from jax.sharding import PartitionSpec as P

GRID = 96
ITERS = 2
SIDE = 2 * (GRID // 3)
LANES = 128
f32 = jnp.float32
bf16 = jnp.bfloat16
highest = lax.Precision.HIGHEST


def split_const(table):
    table = np.asarray(table, np.float32)
    high = table.astype(jnp.bfloat16)
    low = (table - high.astype(np.float32)).astype(jnp.bfloat16)
    return high, low


def phases(rows, cols):
    angle = (np.outer(rows, cols) % GRID) * (2.0 * np.pi / GRID)
    return np.cos(angle) / np.sqrt(GRID), np.sin(angle) / np.sqrt(GRID)


def z_table(bands):
    cos, sin = phases(np.arange(GRID), np.arange(GRID))
    table = np.zeros((GRID, bands, 2, 2, bands, GRID))
    for b in range(bands):
        table[:, b, 0, 0, b] = cos
        table[:, b, 0, 1, b] = -sin
        table[:, b, 1, 0, b] = sin
        table[:, b, 1, 1, b] = cos
    return table.reshape(GRID * bands * 2, 2 * bands * GRID)


def square_freqs():
    return (np.arange(SIDE) - SIDE // 2) % GRID


def y_table():
    cos, sin = phases(np.arange(GRID), square_freqs())
    return np.block([[cos, -sin], [sin, cos]])


def x_table():
    cos, sin = phases(square_freqs(), np.arange(GRID))
    table = np.zeros((SIDE, 2 * LANES))
    table[:, :GRID] = cos
    table[:, LANES : LANES + GRID] = sin
    return table


def x_back_table():
    cos, sin = phases(np.arange(GRID), square_freqs())
    table = np.zeros((LANES, 4 * SIDE))
    table[:GRID] = np.concatenate([cos, cos, sin, sin], axis=1)
    return table


def split(x):
    high = x.astype(bf16)
    return high, (x - high.astype(f32)).astype(bf16)


def dot(a, b):
    return jnp.dot(a, b, preferred_element_type=f32)


def left(table_hi, table_lo, x):
    high, low = split(x)
    return dot(table_hi, high) + (dot(table_hi, low) + dot(table_lo, high))


def right(x, table_hi, table_lo):
    high, low = split(x)
    return dot(high, table_hi) + (dot(low, table_hi) + dot(high, table_lo))


def params(grid_dims=0):
    semantics = ("arbitrary",) * grid_dims if grid_dims else None
    return pltpu.CompilerParams(
        vmem_limit_bytes=56 * 1024 * 1024, dimension_semantics=semantics
    )


def z_inverse_kernel(coef, t_hi, t_lo, out):
    value = coef[...]
    out[...] = dot(t_hi[...], value) + dot(t_lo[...], value)


def z_inverse(coef, table):
    return pl.pallas_call(
        z_inverse_kernel,
        out_shape=jax.ShapeDtypeStruct(coef.shape, f32),
        compiler_params=params(),
        name="z_inverse",
    )(coef, *table)


def intersect_kernel(bands, recv, occ, b_hi, b_lo, image, parts):
    image[...] = left(b_hi[...], b_lo[...], recv[...])
    total = occ.shape[0] * bands
    sticks = recv.shape[1]

    def lanes(x):
        row = jnp.sum(x, axis=0, keepdims=True)
        return sum(row[:, k : k + LANES] for k in range(0, sticks, LANES))

    for n in range(bands):
        re = image[n * GRID : (n + 1) * GRID, :]
        im = image[(bands + n) * GRID : (bands + n + 1) * GRID, :]
        for m in range(total):
            group, own = m // bands, m % bands
            o_re = occ[group, 0, own].astype(f32)
            o_im = occ[group, 1, own].astype(f32)
            at = m * bands + n
            parts[at : at + 1, :] = lanes(o_re * re + o_im * im)
            at = at + total * bands
            parts[at : at + 1, :] = lanes(o_re * im - o_im * re)


def planes_kernel(mode, bands, recv, pot, row, col1, col2, xt_hi, xt_lo, yt_hi, yt_lo, yb_hi, yb_lo, xb_hi, xb_lo, *rest):
    groups, rows, sticks = recv.shape
    planes = rows // (2 * bands)
    count = planes * bands
    rest = list(rest)
    if mode == "next":
        first, psi_field, ratio = rest[:3]
        rest = rest[3:]
    if mode == "local":
        psi_field = rest[0]
        rest = rest[1:]
    spread = rest[-1]
    for g in range(groups):
        at = g * sticks
        mask = row[:, at : at + sticks]
        value = recv[g]
        high = value.astype(bf16).astype(f32)
        low = value - high
        for part, piece in enumerate((high, low)):
            for r in range(rows):
                to = (part * rows + r) * SIDE
                spread[to : to + SIDE, at : at + sticks] = (mask * piece[r : r + 1, :]).astype(bf16)
    both = dot(spread[...], col1[...])
    half = rows * SIDE
    square = both[:half] + both[half:]
    wide = right(square, xt_hi[...], xt_lo[...])
    fields = []
    for n in range(count):
        re = wide[(2 * n) * SIDE : (2 * n + 1) * SIDE]
        im = wide[(2 * n + 1) * SIDE : (2 * n + 2) * SIDE]
        fields.append(
            jnp.concatenate([re[:, :LANES] - im[:, LANES:], re[:, LANES:] + im[:, :LANES]], axis=0)
        )
    field = left(yt_hi[...], yt_lo[...], jnp.concatenate(fields, axis=1))
    if mode == "next":
        quad, dens = rest[:2]
    elif mode == "local":
        field_out, quad, dens, back = rest[:4]
        field_out[0] = field
    else:
        field_out, back = rest[:2]
        field_out[0] = field
    if mode != "dv":
        sums = [jnp.zeros((1, LANES), f32) for _ in range(bands)]
    products = []
    for n in range(count):
        p, b = n // bands, n % bands
        at = n * LANES
        re = field[:GRID, at : at + LANES]
        im = field[GRID:, at : at + LANES]
        v = pot[p]
        if mode == "next":
            re = re + ratio[b] * first[0, :GRID, at : at + LANES]
            im = im + ratio[b] * first[0, GRID:, at : at + LANES]
        v_re, v_im = v * re, v * im
        if mode != "dv":
            dens[p, b] = (
                psi_field[0, :GRID, at : at + LANES] * re + psi_field[0, GRID:, at : at + LANES] * im
            )
            sums[b] = sums[b] + jnp.sum(v_re * re + v_im * im, axis=0, keepdims=True)
        products.append(jnp.concatenate([v_re, v_im], axis=0))
    if mode != "dv":
        quad[0] = jnp.concatenate(sums, axis=0)
    if mode == "next":
        return
    columns = left(yb_hi[...], yb_lo[...], jnp.concatenate(products, axis=1))
    stacked = jnp.concatenate([columns[:, n * LANES : (n + 1) * LANES] for n in range(count)], axis=0)
    wide = right(stacked, xb_hi[...], xb_lo[...])
    squares = []
    for n in range(count):
        re = wide[(2 * n) * SIDE : (2 * n + 1) * SIDE]
        im = wide[(2 * n + 1) * SIDE : (2 * n + 2) * SIDE]
        squares += [re[:, :LANES] + im[:, LANES:], im[:, :LANES] - re[:, LANES:]]
    square = jnp.concatenate(squares, axis=0)
    high = square.astype(bf16).astype(f32)
    lane = lax.broadcasted_iota(jnp.int32, square.shape, 1)
    pair = jnp.where(lane < SIDE, high, square - high).astype(bf16)
    for g in range(groups):
        at = g * sticks
        mask = row[:, at : at + sticks]
        by_row = dot(pair, col2[:, at : at + sticks])
        for r in range(rows):
            back[g, r : r + 1, :] = jnp.sum(
                by_row[r * SIDE : (r + 1) * SIDE] * mask, axis=0, keepdims=True
            )


def planes_call(mode, recv, pot, maps, tables, groups, bands, extra=()):
    sticks = recv.shape[-1]
    planes = pot.shape[0]
    local = planes * 2 * bands
    rows = groups * local
    recv = recv.reshape(groups, -1, sticks)
    step = max(1, 8 // (2 * bands))
    if planes % step:
        step = planes
    steps = planes // step
    width = step * bands * LANES
    whole = lambda a: pl.BlockSpec(a.shape, lambda i: (0,) * a.ndim)
    sticks_spec = pl.BlockSpec((groups, step * 2 * bands, sticks), lambda i: (0, i, 0))
    field_spec = pl.BlockSpec((1, 2 * GRID, width), lambda i: (i, 0, 0))
    field_shape = jax.ShapeDtypeStruct((steps, 2 * GRID, width), f32)
    quad_spec = pl.BlockSpec((1, bands, LANES), lambda i: (i, 0, 0))
    quad_shape = jax.ShapeDtypeStruct((steps, bands, LANES), f32)
    dens_spec = pl.BlockSpec((step, bands, GRID, LANES), lambda i: (i, 0, 0, 0))
    dens_shape = jax.ShapeDtypeStruct((planes, bands, GRID, LANES), f32)
    back_shape = jax.ShapeDtypeStruct((groups, local, sticks), f32)
    in_specs = [sticks_spec, pl.BlockSpec((step, GRID, LANES), lambda i: (i, 0, 0))]
    in_specs += [whole(a) for a in maps] + [whole(a) for a in tables]
    if mode == "dv":
        out_specs, out_shape = [field_spec, sticks_spec], [field_shape, back_shape]
    elif mode == "local":
        in_specs += [field_spec]
        out_specs = [field_spec, quad_spec, dens_spec, sticks_spec]
        out_shape = [field_shape, quad_shape, dens_shape, back_shape]
    else:
        in_specs += [field_spec, field_spec, pl.BlockSpec(memory_space=pltpu.SMEM)]
        out_specs, out_shape = [quad_spec, dens_spec], [quad_shape, dens_shape]
    result = pl.pallas_call(
        functools.partial(planes_kernel, mode, bands),
        grid=(steps,),
        in_specs=in_specs,
        out_specs=out_specs,
        out_shape=out_shape,
        scratch_shapes=[pltpu.VMEM((2 * step * 2 * bands * SIDE, groups * sticks), bf16)],
        compiler_params=params(1),
        name="planes_" + mode,
    )(recv, pot, *maps, *tables, *extra)
    if mode != "next":
        result = list(result)
        result[-1] = result[-1].reshape(rows, sticks)
    return result


def project(beta, vector, bands, acc, chunk):
    count = beta.shape[1]

    def fold(x):
        parts = [x[k : k + 8, l : l + LANES] for k in range(0, x.shape[0], 8) for l in range(0, x.shape[1], LANES)]
        while len(parts) > 1:
            parts = [sum(parts[k : k + 2][1:], parts[k]) for k in range(0, len(parts), 2)]
        return parts[0]

    def body(k, carry):
        for u in range(chunk):
            j = k * chunk + u
            b_re, b_im = beta[0, j], beta[1, j]
            for b in range(bands):
                re, im = vector[0][b], vector[1][b]
                acc[j, b] += fold(b_re * re + b_im * im)
                acc[j, bands + b] += fold(b_re * im - b_im * re)
        return carry

    lax.fori_loop(0, count // chunk, body, 0)


def emit(acc, projected, vec, out, t_hi, t_lo):
    projected[...] = jnp.sum(acc[...], axis=2)
    out[...] = left(t_hi[...], t_lo[...], vec[...])


def tile_sums(x):
    row = jnp.sum(x, axis=0, keepdims=True)
    return sum(row[:, k : k + LANES] for k in range(0, x.shape[1], LANES))


def rhs_kernel(bands, parts, occ, image, diag, beta, t_hi, t_lo, vec_out, stats, projected, out, vec, acc):
    step = pl.program_id(0)
    last = pl.num_programs(0) - 1
    zt = image.shape[2]
    total = occ.shape[0] * bands

    @pl.when(step == 0)
    def _():
        acc[...] = jnp.zeros_like(acc)
        stats[...] = jnp.zeros_like(stats)

    vector = [[], []]
    for n in range(bands):
        re, im = -image[0, n], -image[1, n]
        for m in range(total):
            group, own = m // bands, m % bands
            o_re = occ[group, 0, own].astype(f32)
            o_im = occ[group, 1, own].astype(f32)
            at = m * bands + n
            i_re = parts[0, at]
            i_im = parts[0, at + total * bands]
            re = re + (o_re * i_re - o_im * i_im)
            im = im + (o_re * i_im + o_im * i_re)
        vector[0].append(re)
        vector[1].append(im)
    for n in range(bands):
        d = diag[n]
        sq = vector[0][n] * vector[0][n] + vector[1][n] * vector[1][n]
        stats[0, n : n + 1, :] += tile_sums(sq)
        stats[1, n : n + 1, :] += tile_sums(d * sq)
        for c in range(2):
            vec_out[c, n] = vector[c][n]
            vec[pl.ds((c * bands + n) * GRID + step * zt, zt), :] = vector[c][n]
    project(beta, vector, bands, acc, 4)

    @pl.when(step == last)
    def _():
        emit(acc, projected, vec, out, t_hi, t_lo)


def update_kernel(bands, coupled, alpha, recv, p0, diag, beta, b_hi, b_lo, t_hi, t_lo, vec_out, stats, projected, out, vec, local, acc):
    step = pl.program_id(0)
    last = pl.num_programs(0) - 1
    zt = p0.shape[2]

    @pl.when(step == 0)
    def _():
        acc[...] = jnp.zeros_like(acc)
        stats[...] = jnp.zeros_like(stats)
        local[...] = left(b_hi[...], b_lo[...], recv[...])

    first = []
    for c in range(2):
        for n in range(bands):
            at = pl.multiple_of((c * bands + n) * GRID + step * zt, 8)
            first.append(diag[n] * p0[c, n] + local[pl.ds(at, zt), :])

    def body(k, carry):
        for u in range(2):
            j = k * 2 + u
            b_re, b_im = beta[0, j], beta[1, j]
            new = [None] * (2 * bands)
            for n in range(bands):
                w_re, w_im = coupled[n, j], coupled[bands + n, j]
                new[n] = carry[n] + (b_re * w_re - b_im * w_im)
                new[bands + n] = carry[bands + n] + (b_re * w_im + b_im * w_re)
            carry = tuple(new)
        return carry

    image = lax.fori_loop(0, beta.shape[1] // 2, body, tuple(first))
    vector = [[], []]
    for c in range(2):
        for n in range(bands):
            value = p0[c, n] - alpha[n] * image[c * bands + n]
            vector[c].append(value)
            vec_out[c, n] = value
            at = pl.multiple_of((c * bands + n) * GRID + step * zt, 8)
            vec[pl.ds(at, zt), :] = value
    for n in range(bands):
        d = diag[n]
        sq = vector[0][n] * vector[0][n] + vector[1][n] * vector[1][n]
        cross = vector[0][n] * p0[0, n] + vector[1][n] * p0[1, n]
        stats[0, n : n + 1, :] += tile_sums(sq)
        stats[1, n : n + 1, :] += tile_sums(d * sq)
        stats[2, n : n + 1, :] += tile_sums(d * cross)
    project(beta, vector, bands, acc, 4)

    @pl.when(step == last)
    def _():
        emit(acc, projected, vec, out, t_hi, t_lo)


def frequency(index):
    return (index + GRID // 2) % GRID - GRID // 2


def per_device(psi, vloc, dv, beta, dij, atom_type, stick_xy, band_shift, *, groups):
    bands, sticks = psi.shape[1], psi.shape[3]
    nproj = beta.shape[1]
    planes = vloc.shape[0]
    all_sticks = stick_xy.shape[0]
    flat = (2 * bands * GRID, sticks)
    shaped = (2, bands, GRID, sticks)
    table = z_table(bands)
    t_inv = [jnp.asarray(a) for a in split_const(table)]
    t_fwd = [jnp.asarray(a) for a in split_const(table.T)]
    tables = []
    for item in (x_table(), y_table(), y_table().T, x_back_table()):
        tables += [jnp.asarray(a) for a in split_const(item)]
    slots = jnp.arange(SIDE, dtype=jnp.int32)
    row_slot = frequency(stick_xy // GRID) + SIDE // 2
    col_slot = frequency(stick_xy % GRID) + SIDE // 2
    row_hot = (slots[:, None] == row_slot[None, :]).astype(f32)
    col_hot = (col_slot[:, None] == slots[None, :]).astype(bf16)
    twice = jnp.arange(2 * SIDE, dtype=jnp.int32) % SIDE
    col_twice = (twice[:, None] == col_slot[None, :]).astype(bf16)
    maps = (row_hot, col_hot, col_twice)

    def grid_of(field):
        return jnp.pad(field.reshape(planes, GRID, GRID), ((0, 0), (0, 0), (0, LANES - GRID)))

    def swap(x):
        return lax.all_to_all(x, "ga", split_axis=0, concat_axis=0, tiled=True)

    def pack(values, width):
        line = jnp.concatenate([v.reshape(-1) for v in values])
        tile = 8 * width
        line = jnp.pad(line, (0, -line.shape[0] % tile)).reshape(1, -1, width)
        return jnp.broadcast_to(line, (groups,) + line.shape[1:])

    def unpack(rows, values):
        line = jnp.sum(rows, axis=0).reshape(-1)
        out, at = [], 0
        for v in values:
            out.append(line[at : at + v.size].reshape(v.shape))
            at += v.size
        return out

    def group_sum(*values):
        return unpack(swap(pack(values, LANES)), values)

    def swap_with(x, *values):
        x = x.reshape(groups, -1, sticks)
        both = swap(jnp.concatenate([x, pack(values, sticks)], axis=1))
        return both, unpack(both[:, x.shape[1] :], values)

    start = lax.axis_index("ga") * sticks
    own_xy = lax.dynamic_slice_in_dim(stick_xy, start, sticks)
    freq_z = frequency(jnp.arange(GRID, dtype=jnp.int32))
    summed = (
        freq_z[:, None] ** 2
        + (frequency(own_xy // GRID) ** 2 + frequency(own_xy % GRID) ** 2)[None, :]
    )
    kinetic = summed.astype(f32) * (4.0 / (GRID * GRID))
    diag = kinetic[None] + band_shift[:, None, None]
    onehot = (atom_type[:, None] == jnp.arange(dij.shape[0], dtype=jnp.int32)[None, :]).astype(f32)
    selected = jnp.einsum("at,tij->aij", onehot, dij, precision=highest)

    def couple(projected):
        parts = projected.reshape(2 * bands, selected.shape[0], selected.shape[1])
        return jnp.einsum("aij,caj->cai", selected, parts, precision=highest).reshape(2 * bands, nproj)

    nb = lax.axis_size("band")
    shifts = [[(i, (i + k) % nb) for i in range(nb)] for k in range(1, nb)]
    occ = jnp.stack([psi] + [lax.ppermute(psi, "band", ring) for ring in shifts])
    dv_grid, vloc_grid = grid_of(dv), grid_of(vloc)
    along = swap(z_inverse(psi.reshape(flat), t_inv))
    psi_field, back = planes_call("dv", along, dv_grid, maps, tables, groups, bands)
    pairs = 2 * occ.shape[0] * bands * bands
    image, parts = pl.pallas_call(
        functools.partial(intersect_kernel, bands),
        out_shape=[jax.ShapeDtypeStruct(flat, f32), jax.ShapeDtypeStruct((pairs, LANES), f32)],
        compiler_params=params(),
        name="intersects",
    )(swap(back), occ, *t_fwd)
    inv_norm = 1.0 / (2.0 * GRID * all_sticks)
    intersect = (group_sum(jnp.sum(parts, axis=1))[0] * inv_norm)[None]

    zt = 16
    steps = GRID // zt
    whole = lambda a: pl.BlockSpec(a.shape, lambda i: (0,) * a.ndim)
    smem = pl.BlockSpec(memory_space=pltpu.SMEM)
    vec_spec = pl.BlockSpec((2, bands, zt, sticks), lambda i: (0, 0, i, 0))
    occ_spec = pl.BlockSpec((occ.shape[0], 2, bands, zt, sticks), lambda i: (0, 0, 0, i, 0))
    diag_spec = pl.BlockSpec((bands, zt, sticks), lambda i: (0, i, 0))
    beta_spec = pl.BlockSpec((2, nproj, zt, sticks), lambda i: (0, 0, i, 0))
    stats_shape = jax.ShapeDtypeStruct((3, bands, LANES), f32)
    proj_shape = jax.ShapeDtypeStruct((nproj, 2 * bands, LANES), f32)
    flat_shape = jax.ShapeDtypeStruct(flat, f32)
    outs = [jax.ShapeDtypeStruct(shaped, f32), stats_shape, proj_shape, flat_shape]
    out_specs = [vec_spec, whole(stats_shape), whole(proj_shape), whole(flat_shape)]
    acc_scratch = pltpu.VMEM((nproj, 2 * bands, 8, LANES), f32)

    p0, stats0, proj0, along = pl.pallas_call(
        functools.partial(rhs_kernel, bands),
        grid=(steps,),
        in_specs=[smem, occ_spec, vec_spec, diag_spec, beta_spec, whole(t_inv[0]), whole(t_inv[1])],
        out_specs=out_specs,
        out_shape=outs,
        scratch_shapes=[pltpu.VMEM(flat, f32), acc_scratch],
        compiler_params=params(1),
        name="rhs",
    )(intersect, occ, image.reshape(shaped), diag, beta, *t_inv)
    p0_field, quad0, dens0, back = planes_call(
        "local", swap(along), vloc_grid, maps, tables, groups, bands, (psi_field,)
    )
    both, (stats0, proj0, quad0) = swap_with(
        back, jnp.sum(stats0, axis=2), jnp.sum(proj0, axis=2).T, jnp.sum(quad0, axis=(0, 2))
    )
    back = both[:, : planes * 2 * bands].reshape(flat)
    coupled0 = couple(proj0)

    def band_dot(a, b):
        return jnp.sum((a * b).reshape(2, bands, nproj), axis=(0, 2))

    rr0 = stats0[0]
    alpha0 = rr0 / (stats0[1] + quad0 + band_dot(proj0, coupled0))
    r1, stats1, proj1, along = pl.pallas_call(
        functools.partial(update_kernel, bands),
        grid=(steps,),
        in_specs=[smem, smem, whole(flat_shape), vec_spec, diag_spec, beta_spec]
        + [whole(t_inv[0])] * 4,
        out_specs=out_specs,
        out_shape=outs,
        scratch_shapes=[pltpu.VMEM(flat, f32), pltpu.VMEM(flat, f32), acc_scratch],
        compiler_params=params(1),
        name="update",
    )(coupled0, alpha0, back, p0, diag, beta, *t_fwd, *t_inv)
    both, (stats1, proj1) = swap_with(along, jnp.sum(stats1, axis=2), jnp.sum(proj1, axis=2).T)
    ratio = stats1[0] / rr0
    quad1, dens1 = planes_call(
        "next", both, vloc_grid, maps, tables, groups, bands, (p0_field, psi_field, ratio)
    )
    quad1 = group_sum(jnp.sum(quad1, axis=(0, 2)))[0]
    spread_ratio = jnp.tile(ratio, 2)[:, None]
    proj_p1 = proj1 + spread_ratio * proj0
    diag1 = stats1[1] + ratio * (2.0 * stats1[2] + ratio * stats0[1])
    alpha1 = stats1[0] / (diag1 + quad1 + band_dot(proj_p1, couple(proj_p1)))
    wide = lambda a: a[None, :, None, None]
    response = wide(alpha1) * r1 + wide(alpha0 + alpha1 * ratio) * p0
    contribution = 4.0 * jnp.sum(wide(alpha0) * dens0 + wide(alpha1) * dens1, axis=1)
    blocks = contribution.reshape(planes, nb, GRID // nb, LANES).transpose(1, 0, 2, 3)
    density = jnp.sum(lax.all_to_all(blocks, "band", split_axis=0, concat_axis=0, tiled=True), axis=0)
    return response, density[:, :, :GRID].reshape(planes, -1)


def solution(mesh):
    placed = (
        P(None, "band", None, "ga"),
        P("ga", None),
        P("ga", None),
        P(None, None, None, "ga"),
        P(),
        P(),
        P(),
        P("band"),
    )
    return jax.shard_map(
        functools.partial(per_device, groups=mesh.shape["ga"]),
        mesh=mesh,
        in_specs=placed,
        out_specs=(P(None, "band", None, "ga"), P("ga", "band")),
        check_vma=False,
    )
```
